256 devices in a mesh: row: 16 (over y, z_hi), col: 16 (over x, z_lo, core).
Axes of the slice: x: 4, y: 4, z: 8 (z_hi: 4, z_lo: 2; z = z_hi * 2 + z_lo), core: 2. Of those that a mesh axis runs over, the one named last changes fastest.
Arguments:
- pair_rep: bfloat16 [2048, 2048, 128], P('row', 'col'), may hold values from -8 to 8
- row_ids: int32 [32], P('row'), may hold values from 0 to 2047, as said below
- pad_mask: int32 [2048], P('col'), may hold values from 0 to 1, as said below
- ln_gain: float32 [128], replicated, may hold values from 0.25 to 1.75
- ln_bias: float32 [128], replicated, may hold values from -2 to 2
- w_query: bfloat16 [128, 128], replicated, may hold values from -2 to 2
- w_key: bfloat16 [128, 128], replicated, may hold values from -2 to 2
- w_value: bfloat16 [128, 128], replicated, may hold values from -0.5 to 0.5
- w_gate: bfloat16 [128, 128], replicated, may hold values from -0.5 to 0.5
- gate_bias: float32 [128], replicated, may hold values from -4 to 4
- w_bias: bfloat16 [128, 4], replicated, may hold values from -0.5 to 0.5
- w_out: bfloat16 [128, 128], replicated, may hold values from -0.5 to 0.5
Outputs:
- update: bfloat16 [32, 2048, 128], P('col', 'row')
The draws below stay inside these ranges and needn't reach their ends.
Inputs may be any that keep to these rules, and one draw needn't show every extreme that they name: `row_ids`: entries t * 2 to t * 2 + 1 are distinct and lie in [t * 128, (t + 1) * 128). `pad_mask`: A prefix of the tokens is real and the rest is padding; the first 513 tokens are real.
All inputs are finite; a program needn't handle non-finite values.
Results may differ from the reference program's by a relative error of at most 0.023.
Values may be sent and summed in bfloat16 or wider, within the bound.
No kernel may reach another device: no remote copies, remote signals or barrier semaphores. Data moves between devices by JAX's collectives and lax.ppermute only.
A program may use at most 128 MiB of HBM per device.

```python
import math
import jax
import jax.numpy as jnp
from jax import lax

CZ = 128
HEADS = 4
HEAD_DIM = 32
ROW_BLOCK = 128
ROWS_DEV = 2
TOKENS = 2048
SELECTED = 32


def draw_row_ids(key, part):
    groups = SELECTED // ROWS_DEV
    keys = jax.random.split(jax.random.fold_in(key, 11), groups)
    picks = jax.vmap(lambda single: jax.random.permutation(single, ROW_BLOCK)[:ROWS_DEV])(keys)
    picks = picks + (jnp.arange(groups, dtype=jnp.int32) * ROW_BLOCK)[:, None]
    return picks.reshape(-1).astype(jnp.int32)


def draw_pad_mask(key, part):
    length = jax.random.randint(jax.random.fold_in(key, 23), (), TOKENS // 4 + 1, TOKENS + 1)
    return (jnp.arange(TOKENS, dtype=jnp.int32) < length).astype(jnp.int32)


def unit_direction(key):
    raw = jnp.clip(jax.random.normal(jax.random.fold_in(key, 101), (CZ,), jnp.float32), -3.0, 3.0)
    raw = raw - jnp.mean(raw)
    return raw / jnp.sqrt(jnp.sum(raw * raw))


def head_vector(key):
    raw = jax.random.normal(jax.random.fold_in(key, 211), (HEADS, HEAD_DIM), jnp.float32)
    raw = raw / jnp.sqrt(jnp.sum(raw * raw, axis=1, keepdims=True))
    strength = 280.0 / CZ * (0.8 + 0.2 * jnp.arange(HEADS, dtype=jnp.float32) / max(HEADS - 1, 1))
    radius = jnp.sqrt(strength * math.sqrt(HEAD_DIM))
    return (raw * radius[:, None]).reshape(HEADS * HEAD_DIM)


def projection_weight(key, salt):
    direction = unit_direction(key)
    along = head_vector(key)
    sub = jax.random.fold_in(key, salt)
    base = jnp.clip(jax.random.normal(sub, (CZ, HEADS * HEAD_DIM), jnp.float32), -4.0, 4.0) / math.sqrt(CZ)
    return jnp.clip(base + direction[:, None] * along[None, :], -2.0, 2.0).astype(jnp.bfloat16)


def draw_w_query(key, part):
    return projection_weight(key, 41)


def draw_w_key(key, part):
    return projection_weight(key, 43)


def draw_ln_bias(key, part):
    direction = unit_direction(key)
    sub = jax.random.fold_in(key, 31)
    raw = jnp.clip(0.5 * jax.random.normal(sub, (CZ,), jnp.float32), -1.5, 1.5)
    return raw - jnp.sum(raw * direction) * direction


def noise_block(key, shape, direction):
    raw = jnp.clip(jax.random.normal(key, shape, jnp.float32), -4.0, 4.0)
    return raw - jnp.sum(raw * direction, axis=-1, keepdims=True) * direction


def draw_pair_rep(key, part):
    direction = unit_direction(key)
    base_key = jax.random.fold_in(key, 53)

    def one_block(index):
        sub = jax.random.fold_in(base_key, index)
        block = noise_block(sub, (TOKENS // 16, TOKENS, CZ), direction)
        return jnp.clip(block, -8.0, 8.0).astype(jnp.bfloat16)
    full = lax.map(one_block, jnp.arange(16, dtype=jnp.int32)).reshape(TOKENS, TOKENS, CZ)
    row_ids = draw_row_ids(key, part)
    count = 3
    picks = jax.random.permutation(jax.random.fold_in(key, 61), SELECTED)[:count]
    planted_rows = row_ids[picks]
    spots = jax.random.permutation(jax.random.fold_in(key, 67), TOKENS // 4)[:6]
    cosines = jnp.array([1.0, 0.993, 0.986, 0.8, 0.65, 0.5], jnp.float32)
    sines = jnp.sqrt(1.0 - cosines * cosines)
    extra = noise_block(jax.random.fold_in(key, 71), (count, 6, CZ), direction)
    planted = cosines[None, :, None] * math.sqrt(CZ) * direction[None, None, :] + sines[None, :, None] * extra
    planted = jnp.clip(planted, -8.0, 8.0).astype(jnp.bfloat16)
    return full.at[planted_rows[:, None], spots[None, :]].set(planted)


def noise(stream_key, extent, scale, limit, held_as=jnp.bfloat16):
    values = scale * jax.random.normal(stream_key, extent, jnp.float32)
    return jnp.clip(values, min=-limit, max=limit).astype(held_as)


def setup_inputs(seed: int = 0) -> dict:
    seeds = jax.random.split(jax.random.key(seed), 13)
    pair_rep = draw_pair_rep(jax.random.fold_in(seeds[12], 71), 0)
    row_ids = draw_row_ids(jax.random.fold_in(seeds[12], 71), 0)
    pad_mask = draw_pad_mask(jax.random.fold_in(seeds[12], 71), 0)
    ln_gain = jnp.clip(1.0 + 0.15 * jax.random.normal(seeds[3], (CZ,), jnp.float32), 0.25, 1.75)
    ln_bias = draw_ln_bias(jax.random.fold_in(seeds[12], 71), 0)
    w_query = draw_w_query(jax.random.fold_in(seeds[12], 71), 0)
    w_key = draw_w_key(jax.random.fold_in(seeds[12], 71), 0)
    w_value = noise(seeds[7], (CZ, HEADS * HEAD_DIM), CZ ** -0.5, 0.5)
    w_gate = noise(seeds[8], (CZ, HEADS * HEAD_DIM), CZ ** -0.5, 0.5)
    gate_bias = noise(seeds[9], (HEADS * HEAD_DIM,), 1.0, 4.0, jnp.float32)
    w_bias = noise(seeds[10], (CZ, HEADS), CZ ** -0.5, 0.5)
    w_out = noise(seeds[11], (HEADS * HEAD_DIM, CZ), (HEADS * HEAD_DIM) ** -0.5, 0.5)
    return dict(pair_rep=pair_rep, row_ids=row_ids, pad_mask=pad_mask, ln_gain=ln_gain, ln_bias=ln_bias, w_query=w_query, w_key=w_key, w_value=w_value, w_gate=w_gate, gate_bias=gate_bias, w_bias=w_bias, w_out=w_out)


def layer_norm(values, ln_gain, ln_bias):
    values = values.astype(jnp.float32)
    centre = lax.optimization_barrier(jnp.mean(values, axis=-1, keepdims=True))
    spread = lax.optimization_barrier(jnp.mean((values - centre) ** 2, axis=-1, keepdims=True))
    return ((values - centre) * lax.rsqrt(spread + 1e-05) * ln_gain + ln_bias).astype(jnp.bfloat16)

def project(normed, weight):
    flat = normed.reshape(-1, normed.shape[-1])
    return jnp.dot(flat, weight, preferred_element_type=jnp.float32).reshape(normed.shape[:-1] + (weight.shape[1],))

def reference(pair_rep, row_ids, pad_mask, ln_gain, ln_bias, w_query, w_key, w_value, w_gate, gate_bias, w_bias, w_out):
    tokens = pair_rep.shape[0]
    heads = w_bias.shape[1]
    width = w_query.shape[1]
    head_dim = width // heads
    block_count = tokens // 16

    def bias_block(block):
        normed = layer_norm(block, ln_gain, ln_bias)
        return jnp.einsum('jkc,ch->hjk', normed.astype(jnp.float32), w_bias.astype(jnp.float32))
    blocks = pair_rep.reshape(block_count, tokens // block_count, tokens, pair_rep.shape[2])
    pair_bias = lax.map(bias_block, blocks)
    pair_bias = jnp.transpose(pair_bias, (1, 0, 2, 3)).reshape(heads, tokens, tokens)
    chosen = layer_norm(pair_rep[row_ids.astype(jnp.int32)], ln_gain, ln_bias)
    query = (project(chosen, w_query) / jnp.sqrt(jnp.float32(head_dim))).astype(jnp.bfloat16)
    key_rows = project(chosen, w_key).astype(jnp.bfloat16)
    value_rows = project(chosen, w_value).astype(jnp.bfloat16)
    gate = jax.nn.sigmoid(project(chosen, w_gate) + gate_bias).astype(jnp.bfloat16)
    key_live = pad_mask > 0

    def attend_row(items):
        query_row, key_row, value_row = items
        query_heads = query_row.reshape(tokens, heads, head_dim).astype(jnp.float32)
        key_heads = key_row.reshape(tokens, heads, head_dim).astype(jnp.float32)
        value_heads = value_row.reshape(tokens, heads, head_dim).astype(jnp.float32)
        scores = jnp.einsum('jhd,khd->hjk', query_heads, key_heads) + pair_bias
        scores = jnp.where(key_live[None, None, :], scores, jnp.float32(-1000000000.0))
        peak = lax.optimization_barrier(jnp.max(scores, axis=-1, keepdims=True))
        expo = jnp.exp(scores - peak)
        totals = lax.optimization_barrier(jnp.sum(expo, axis=-1))
        probs = expo.astype(jnp.bfloat16).astype(jnp.float32)
        summed = jnp.einsum('hjk,khd->hjd', probs, value_heads) / totals[..., None]
        return jnp.transpose(summed, (1, 0, 2)).reshape(tokens, width)
    attended = lax.map(attend_row, (query, key_rows, value_rows))
    gated = (gate.astype(jnp.float32) * attended).astype(jnp.bfloat16)
    return project(gated, w_out).astype(jnp.bfloat16)
```

```python
import jax
import jax.numpy as jnp
from jax import lax
from jax.sharding import PartitionSpec as P


MASKED = -1e30
STATS = 16
AXES = ("row", "col")


def layer_norm(values, ln_gain, ln_bias):
    values = values.astype(jnp.float32)
    centre = jnp.mean(values, axis=-1, keepdims=True)
    spread = jnp.mean((values - centre) ** 2, axis=-1, keepdims=True)
    return ((values - centre) * lax.rsqrt(spread + 1e-05) * ln_gain + ln_bias).astype(jnp.bfloat16)


def moves(target):
    pairs = []
    for i in range(256):
        y, h, x, q = i // 64, i // 16 % 4, i // 4 % 4, i % 4
        a, b, c, d = target(y, h, x, q)
        pairs.append((i, ((a % 4 * 4 + b % 4) * 4 + c % 4) * 4 + d % 4))
    return pairs


def three_terms(value):
    def rounded(v):
        return lax.reduce_precision(v, 8, 7)

    high = rounded(value)
    middle = rounded(value - high)
    return high, middle, rounded(value - high - middle)


def body(
    pair_rep,
    row_ids,
    pad_mask,
    ln_gain,
    ln_bias,
    w_query,
    w_key,
    w_value,
    w_gate,
    gate_bias,
    w_bias,
    w_out,
):
    block = pair_rep.shape[0]
    heads = w_bias.shape[1]
    width = w_query.shape[1]
    head_dim = width // heads
    row, col = lax.axis_index("row"), lax.axis_index("col")
    y, h, x, q = row // 4, row % 4, col // 4, col % 4
    chosen = jnp.take(pair_rep, row_ids - row * block, axis=0)
    piece = layer_norm(chosen, ln_gain, ln_bias)
    low = [
        lax.ppermute(piece, AXES, moves(lambda y, h, x, q, i=i: (y, q + i, x, h)))
        for i in range(4)
    ]

    normed = layer_norm(pair_rep, ln_gain, ln_bias)
    bias = jnp.einsum("jkc,ch->hjk", normed, w_bias, preferred_element_type=jnp.float32)
    bias = jnp.where((pad_mask > 0)[None, None, :], bias, jnp.float32(MASKED))
    other = lax.ppermute(bias, "col", [(i, i ^ 2) for i in range(16)])
    near = jnp.stack([bias, other])
    far = lax.ppermute(near, "col", [(i, i ^ 1) for i in range(16)])
    bias_all = jnp.concatenate([near, far])

    own = jnp.stack(low)
    rows_kv = [own] + [
        lax.ppermute(own, AXES, moves(lambda y, h, x, q, s=s: (y + s, h, x, q)))
        for s in (1, 2, 3)
    ]
    rows_q = [
        lax.ppermute(low[0], AXES, moves(lambda y, h, x, q, s=s: (x, h, y + s, q)))
        for s in range(4)
    ]
    rows_kv = jnp.stack(rows_kv)

    flips = [((h - i) % 4) ^ q for i in range(4)]
    slots = [(f >> 1) | ((f & 1) << 1) for f in flips]
    bias_here = jnp.concatenate(
        [lax.dynamic_index_in_dim(bias_all, s, 0, keepdims=False) for s in slots], axis=-1
    )

    def attend(s):
        kv = lax.dynamic_index_in_dim(rows_kv, (y - x + s) % 4, 0, keepdims=False)
        kv = jnp.transpose(kv, (1, 0, 2, 3)).reshape(2, 4 * block, width)
        query = jnp.dot(rows_q[s], w_query, preferred_element_type=jnp.float32)
        query = (query / jnp.sqrt(jnp.float32(head_dim))).astype(jnp.bfloat16)
        key = jnp.dot(kv, w_key, preferred_element_type=jnp.float32).astype(jnp.bfloat16)
        value = jnp.dot(kv, w_value, preferred_element_type=jnp.float32).astype(jnp.bfloat16)
        query = query.reshape(2, block, heads, head_dim)
        key = key.reshape(2, 4 * block, heads, head_dim)
        value = value.reshape(2, 4 * block, heads, head_dim)
        scores = jnp.einsum("tjhd,tkhd->thjk", query, key, preferred_element_type=jnp.float32)
        scores = scores + bias_here[None]
        peak = jnp.max(scores, axis=-1)
        expo = jnp.exp(scores - peak[..., None])
        totals = jnp.sum(expo, axis=-1)
        summed = jnp.einsum(
            "thjk,tkhd->tjhd",
            expo.astype(jnp.bfloat16),
            value,
            preferred_element_type=jnp.float32,
        ).reshape(2, block, width)
        stats = jnp.concatenate([*three_terms(peak), totals], axis=1)
        return jnp.concatenate([summed, stats], axis=1).astype(jnp.bfloat16)

    parts = []
    for s in (2, 1, 3, 0):
        part = attend(s)
        if s:
            part = lax.ppermute(part, AXES, moves(lambda y, h, x, q, s=s: (y, h, x - s, q)))
        parts.append(part)
    parts = jnp.stack(parts).astype(jnp.float32)
    summed = parts[:, :, :block].reshape(4, 2, block, heads, head_dim)
    stats = parts[:, :, block:].reshape(4, 2, 4, heads, block)
    peak = stats[:, :, 0] + stats[:, :, 1] + stats[:, :, 2]
    factor = jnp.exp(peak - jnp.max(peak, axis=0))
    totals = jnp.sum(factor * stats[:, :, 3], axis=0)
    factor = jnp.swapaxes(factor / totals, 2, 3)
    attended = jnp.sum(summed * factor[..., None], axis=0).reshape(2, block, width)
    gate = jnp.dot(rows_q[0], w_gate, preferred_element_type=jnp.float32) + gate_bias
    gate = jax.nn.sigmoid(gate).astype(jnp.bfloat16)
    gated = (gate.astype(jnp.float32) * attended).astype(jnp.bfloat16)
    return jnp.dot(gated, w_out, preferred_element_type=jnp.float32).astype(jnp.bfloat16)


def solution(mesh):
    return jax.shard_map(
        body,
        mesh=mesh,
        in_specs=(P("row", "col", None), P("row"), P("col")) + (P(),) * 9,
        out_specs=P("col", "row", None),
        check_vma=False,
    )
```

```python
import jax
import jax.numpy as jnp
from jax import lax
from jax.experimental import pallas as pl
from jax.experimental.pallas import tpu as pltpu
from jax.sharding import PartitionSpec as P


MASKED = -1e30
STATS = 16
BIAS_ROWS = 16
AXES = ("row", "col")
F32 = jnp.float32
BF16 = jnp.bfloat16
VMEM = pltpu.VMEM


def params(mib=16):
    return pltpu.CompilerParams(vmem_limit_bytes=mib << 20)


def cost(flops, moved, exps=0):
    return pl.CostEstimate(flops=flops, bytes_accessed=moved, transcendentals=exps)


def whole():
    return pl.BlockSpec(memory_space=VMEM)


def layer_norm(values, ln_gain, ln_bias):
    values = values.astype(F32)
    values = values - jnp.mean(values, axis=-1, keepdims=True)
    spread = jnp.mean(values * values, axis=-1, keepdims=True)
    return (values * lax.rsqrt(spread + 1e-05) * ln_gain + ln_bias).astype(BF16)


def fetch_kernel(row_ids, pair_rep, ln_gain, ln_bias, out, ids, rows, gain, shift, sems):
    copies = [
        pltpu.make_async_copy(row_ids, ids, sems.at[0]),
        pltpu.make_async_copy(ln_gain, gain, sems.at[1]),
        pltpu.make_async_copy(ln_bias, shift, sems.at[2]),
    ]
    for copy in copies:
        copy.start()
    copies[0].wait()
    for t in range(rows.shape[0]):
        at = lax.rem(ids[t], pair_rep.shape[0])
        copies.append(pltpu.make_async_copy(pair_rep.at[at], rows.at[t], sems.at[3 + t]))
        copies[-1].start()
    copies[1].wait()
    copies[2].wait()
    for t in range(rows.shape[0]):
        copies[3 + t].wait()
        out[t] = layer_norm(rows[t], gain[...], shift[...])


def fetch(row_ids, pair_rep, ln_gain, ln_bias):
    _, tokens, width = pair_rep.shape
    count = row_ids.shape[0]
    return pl.pallas_call(
        fetch_kernel,
        in_specs=[pl.BlockSpec(memory_space=pltpu.HBM)] * 4,
        out_specs=whole(),
        out_shape=jax.ShapeDtypeStruct((count, tokens, width), BF16),
        scratch_shapes=[
            pltpu.SMEM((count,), jnp.int32),
            VMEM((count, tokens, width), BF16),
            VMEM((1, width), F32),
            VMEM((1, width), F32),
            pltpu.SemaphoreType.DMA((3 + count,)),
        ],
        compiler_params=params(60),
        cost_estimate=cost(10 * count * tokens * width, 4 * count * tokens * width),
        name="fetch",
    )(row_ids, pair_rep, ln_gain, ln_bias)


def bias_kernel(
    pair_rep, ln_gain, ln_bias, w_bias, pad_mask, out, rows, lifted, gain, shift, weights, live, sems
):
    heads, block, tokens = out.shape
    width = rows.shape[2]
    small = [(ln_gain, gain), (ln_bias, shift), (w_bias, weights), (pad_mask, live)]
    copies = [pltpu.make_async_copy(a, b, sems.at[i]) for i, (a, b) in enumerate(small)]
    for i in range(0, block, BIAS_ROWS):
        part = pl.ds(i, BIAS_ROWS)
        at = len(small) + i // BIAS_ROWS
        copies.append(pltpu.make_async_copy(pair_rep.at[part], rows.at[part], sems.at[at]))
    for copy in copies:
        copy.start()
    for copy in copies[: len(small)]:
        copy.wait()
    plain = weights[...].astype(F32)
    scaled = plain * gain[...]
    high = scaled.astype(BF16).astype(F32)
    at = lax.broadcasted_iota(jnp.int32, (heads * 8, width), 0) % 8
    offset = jnp.sum(plain * shift[...], axis=1, keepdims=True)
    offset = jnp.broadcast_to(offset[:, None], (heads, 8, tokens))
    for part, value in enumerate((high, scaled - high)):
        value = jnp.broadcast_to(value[:, None], (heads, 8, width)).reshape(heads * 8, width)
        for j in range(8):
            placed = jnp.where(at == j, value, 0.0).astype(BF16)
            lifted[j, part * heads * 8 : (part + 1) * heads * 8] = placed
    real = live[...] > 0
    sub = lax.broadcasted_iota(jnp.int32, (8, tokens), 0)

    def eight(group, carry):
        total = jnp.zeros((2 * heads * 8, tokens), F32)
        spread = jnp.zeros((8, tokens), F32)
        for j in range(8):
            values = rows[group * 8 + j].T.astype(F32)
            values = values - jnp.sum(values, axis=0, keepdims=True) * (1.0 / width)
            total += jnp.dot(lifted[j], values.astype(BF16), preferred_element_type=F32)
            squares = jnp.sum(values * values, axis=0, keepdims=True)
            spread = jnp.where(sub == j, squares, spread)
        scale = lax.rsqrt(spread * (1.0 / width) + 1e-05)
        total = total[: heads * 8] + total[heads * 8 :]
        total = total.reshape(heads, 8, tokens) * scale[None] + offset
        out[:, pl.ds(pl.multiple_of(group * 8, 8), 8), :] = jnp.where(real, total, MASKED)
        return carry

    for i in range(0, block, BIAS_ROWS):
        copies[len(small) + i // BIAS_ROWS].wait()
        lax.fori_loop(i // 8, (i + BIAS_ROWS) // 8, eight, 0)


def pair_bias(pair_rep, ln_gain, ln_bias, w_bias, pad_mask):
    block, tokens, width = pair_rep.shape
    heads = w_bias.shape[1]
    return pl.pallas_call(
        bias_kernel,
        in_specs=[pl.BlockSpec(memory_space=pltpu.HBM)] * 5,
        out_specs=whole(),
        out_shape=jax.ShapeDtypeStruct((heads, block, tokens), F32),
        scratch_shapes=[
            VMEM((block, tokens, width), BF16),
            VMEM((8, 2 * heads * 8, width), BF16),
            VMEM((1, width), F32),
            VMEM((1, width), F32),
            VMEM((heads, width), BF16),
            VMEM((1, tokens), jnp.int32),
            pltpu.SemaphoreType.DMA((4 + block // BIAS_ROWS,)),
        ],
        compiler_params=params(60),
        cost_estimate=cost(4 * block * tokens * width, 2 * block * tokens * width),
        name="pair_bias",
    )(pair_rep, ln_gain, ln_bias, w_bias.T, pad_mask.reshape(1, tokens))


def project_kernel(*refs):
    blocks, (w_key, w_value, keys, values) = refs[:-4], refs[-4:]
    block, width = blocks[0].shape[-2:]
    row, col = lax.axis_index("row"), lax.axis_index("col")
    y, h, x, q = row // 4, row % 4, col // 4, col % 4
    places = [(x - y + s + 4) % 4 for s in range(4)]
    flips = [((h - i + 4) % 4) ^ q for i in range(4)]
    places += [(f // 2) + (f % 2) * 2 for f in flips]
    weights = jnp.concatenate([w_key[...], w_value[...]], axis=1)
    for s in range(4):
        for i in range(4):
            for t in range(2):
                both = jnp.dot(blocks[s][i, t], weights, preferred_element_type=F32)
                both = both.astype(BF16)
                at = pl.ds(pl.multiple_of(places[4 + i] * block, block), block)
                keys[places[s], t, :, at] = both[:, :width].T
                values[places[s], t, at, :] = both[:, width:]


def project(blocks, w_key, w_value):
    block, width = blocks[0].shape[-2:]
    return pl.pallas_call(
        project_kernel,
        in_specs=[whole()] * (len(blocks) + 2),
        out_specs=[whole(), whole()],
        out_shape=[
            jax.ShapeDtypeStruct((4, 2, width, 4 * block), BF16),
            jax.ShapeDtypeStruct((4, 2, 4 * block, width), BF16),
        ],
        compiler_params=params(),
        cost_estimate=cost(2 * 4096 * 128 * 256, 3 << 20),
        name="project",
    )(*blocks, w_key, w_value)


def attend_kernel(rows, keys, values, bias_a, bias_b, bias_c, bias_d, w_query, out):
    block, width = rows.shape[1:]
    heads = bias_a.shape[0]
    head_dim = width // heads
    lane = lax.broadcasted_iota(jnp.int32, (block, width), 1)
    for t in range(2):
        query = jnp.dot(rows[t], w_query[...], preferred_element_type=F32)
        query = (query * (head_dim**-0.5)).astype(BF16)
        key = keys[0, t]
        value = jnp.concatenate([values[0, t], jnp.ones((4 * block, width), BF16)], axis=1)
        summed = jnp.zeros((block, width), F32)
        stats = jnp.zeros((block, width), F32)
        for h in range(heads):
            mine = lane // head_dim == h
            part = jnp.where(mine, query, jnp.zeros_like(query))
            scores = jnp.dot(part, key, preferred_element_type=F32)
            bias = [bias_a[h], bias_b[h], bias_c[h], bias_d[h]]
            scores = scores + jnp.concatenate(bias, axis=1)
            peak = jnp.max(scores, axis=1, keepdims=True)
            expo = jnp.exp(scores - peak).astype(BF16)
            result = jnp.dot(expo, value, preferred_element_type=F32)
            summed = jnp.where(mine, result[:, :width], summed)
            total = result[:, width:]
            high = peak.astype(BF16).astype(F32)
            middle = (peak - high).astype(BF16).astype(F32)
            for i, column in enumerate((high, middle, peak - high - middle, total)):
                stats = jnp.where(lane == i * heads + h, column, stats)
        out[t, :block] = summed.astype(BF16)
        out[t, block:] = stats.T[:STATS].astype(BF16)


def attend(s, rows, keys, values, biases, w_query):
    _, block, width = rows.shape
    parts = [pl.BlockSpec((1, *v.shape[1:]), lambda i: (s, 0, 0, 0)) for v in (keys, values)]
    full = [
        pl.BlockSpec(v.shape, lambda i, n=v.ndim: (0,) * n) for v in (rows, *biases, w_query)
    ]
    return pl.pallas_call(
        attend_kernel,
        grid=(1,),
        in_specs=[full[0], *parts, *full[1:]],
        out_specs=pl.BlockSpec((2, block + STATS, width), lambda i: (0, 0, 0)),
        out_shape=jax.ShapeDtypeStruct((2, block + STATS, width), BF16),
        compiler_params=params(),
        cost_estimate=cost(8 * 2 * 128 * 512 * 128 * 2, 2 << 20, 2 * 4 * 128 * 512),
    )(rows, keys, values, *biases, w_query)


def finish_kernel(first, second, third, fourth, rows, w_gate, gate_bias, w_out, out):
    block, width = rows.shape[1:]
    heads = STATS // 4
    head_dim = width // heads
    parts = (first, second, third, fourth)
    source = lax.broadcasted_iota(jnp.int32, (width, 4 * width), 0)
    target = lax.broadcasted_iota(jnp.int32, (width, 4 * width), 1) // head_dim
    meets = (source % STATS == target) & (source < 2 * STATS)
    spreading = jnp.where(meets, 1.0, 0.0).astype(BF16)
    for t in range(2):
        peaks, totals = [], []
        for part in parts:
            stats = part[t, block:].astype(F32)
            peaks.append(stats[:heads] + stats[heads : 2 * heads] + stats[2 * heads : 3 * heads])
            totals.append(stats[3 * heads :])
        overall = jnp.maximum(jnp.maximum(peaks[0], peaks[1]), jnp.maximum(peaks[2], peaks[3]))
        factors = [jnp.exp(peak - overall) for peak in peaks]
        whole_total = sum(f * total for f, total in zip(factors, totals))
        factors = jnp.concatenate([f / whole_total for f in factors], axis=0)
        high = factors.astype(BF16)
        low = (factors - high.astype(F32)).astype(BF16)
        padding = jnp.zeros((width - 2 * STATS, block), BF16)
        factors = jnp.concatenate([high, low, padding], axis=0).T
        wide = jnp.dot(factors, spreading, preferred_element_type=F32)
        attended = jnp.zeros((block, width), F32)
        for p, part in enumerate(parts):
            attended += wide[:, p * width : (p + 1) * width] * part[t, :block].astype(F32)
        gate = jnp.dot(rows[t], w_gate[...], preferred_element_type=F32) + gate_bias[...]
        gate = jax.nn.sigmoid(gate).astype(BF16).astype(F32)
        gated = (gate * attended).astype(BF16)
        out[t] = jnp.dot(gated, w_out[...], preferred_element_type=F32).astype(BF16)


def finish(parts, rows, w_gate, gate_bias, w_out):
    return pl.pallas_call(
        finish_kernel,
        in_specs=[whole()] * 8,
        out_specs=whole(),
        out_shape=jax.ShapeDtypeStruct(rows.shape, BF16),
        compiler_params=params(),
        cost_estimate=cost(4 * 256 * 128 * 128, 1 << 19),
        name="finish",
    )(*parts, rows, w_gate, gate_bias, w_out)


def moves(target):
    pairs = []
    for i in range(256):
        y, h, x, q = i // 64, i // 16 % 4, i // 4 % 4, i % 4
        a, b, c, d = target(y, h, x, q)
        pairs.append((i, ((a % 4 * 4 + b % 4) * 4 + c % 4) * 4 + d % 4))
    return pairs


def send(value, target):
    return lax.ppermute(value, AXES, moves(target))


def body(
    pair_rep,
    row_ids,
    pad_mask,
    ln_gain,
    ln_bias,
    w_query,
    w_key,
    w_value,
    w_gate,
    gate_bias,
    w_bias,
    w_out,
):
    _, _, width = pair_rep.shape
    ln_gain, ln_bias = ln_gain.reshape(1, width), ln_bias.reshape(1, width)
    piece = fetch(row_ids, pair_rep, ln_gain, ln_bias)
    low = []
    for i in range(4):
        low.append(send(piece, lambda y, h, x, q, i=i: (y, q + i, x, h)))

    bias = pair_bias(pair_rep, ln_gain, ln_bias, w_bias, pad_mask)
    bias_z = send(bias, lambda y, h, x, q: (y, h, x, q ^ 2))
    bias_c = send(bias, lambda y, h, x, q: (y, h, x, q ^ 1))
    bias_zc = send(bias_z, lambda y, h, x, q: (y, h, x, q ^ 1))
    biases = (bias, bias_z, bias_c, bias_zc)

    own = jnp.stack(low)
    rows_kv = [own]
    for s in (1, 2, 3):
        rows_kv.append(send(own, lambda y, h, x, q, s=s: (y + s, h, x, q)))
    rows_q = []
    for s in range(4):
        rows_q.append(send(low[0], lambda y, h, x, q, s=s: (x, h, y + s, q)))

    keys, values = project(rows_kv, w_key, w_value)
    parts = []
    for s in (2, 1, 3, 0):
        part = attend(s, rows_q[s], keys, values, biases, w_query)
        if s:
            part = send(part, lambda y, h, x, q, s=s: (y, h, x - s, q))
        parts.append(part)
    return finish(parts, rows_q[0], w_gate, gate_bias.reshape(1, width), w_out)


def solution(mesh):
    return jax.shard_map(
        body,
        mesh=mesh,
        in_specs=(P("row", "col", None), P("row"), P("col")) + (P(),) * 9,
        out_specs=P("col", "row", None),
        check_vma=False,
    )
```

```python
import functools

import jax
import jax.numpy as jnp
from jax import lax
from jax.experimental import pallas as pl
from jax.experimental.pallas import tpu as pltpu
from jax.sharding import PartitionSpec as P


MASKED = -1e30
STATS = 16
BIAS_ROWS = 16
AXES = ("row", "col")
F32 = jnp.float32
BF16 = jnp.bfloat16
VMEM = pltpu.VMEM


def params(mib=16):
    return pltpu.CompilerParams(vmem_limit_bytes=mib << 20)


def cost(flops, moved, exps=0):
    return pl.CostEstimate(flops=flops, bytes_accessed=moved, transcendentals=exps)


def whole():
    return pl.BlockSpec(memory_space=VMEM)


def layer_norm(values, ln_gain, ln_bias):
    values = values.astype(F32)
    values = values - jnp.mean(values, axis=-1, keepdims=True)
    spread = jnp.mean(values * values, axis=-1, keepdims=True)
    return (values * lax.rsqrt(spread + 1e-05) * ln_gain + ln_bias).astype(BF16)


def fetch_kernel(row_ids, pair_rep, ln_gain, ln_bias, out, ids, rows, gain, shift, sems):
    copies = [
        pltpu.make_async_copy(row_ids, ids, sems.at[0]),
        pltpu.make_async_copy(ln_gain, gain, sems.at[1]),
        pltpu.make_async_copy(ln_bias, shift, sems.at[2]),
    ]
    for copy in copies:
        copy.start()
    copies[0].wait()
    for t in range(rows.shape[0]):
        at = lax.rem(ids[t], pair_rep.shape[0])
        copies.append(pltpu.make_async_copy(pair_rep.at[at], rows.at[t], sems.at[3 + t]))
        copies[-1].start()
    copies[1].wait()
    copies[2].wait()
    for t in range(rows.shape[0]):
        copies[3 + t].wait()
        out[t] = layer_norm(rows[t], gain[...], shift[...])


def fetch(row_ids, pair_rep, ln_gain, ln_bias):
    _, tokens, width = pair_rep.shape
    count = row_ids.shape[0]
    return pl.pallas_call(
        fetch_kernel,
        in_specs=[pl.BlockSpec(memory_space=pltpu.HBM)] * 4,
        out_specs=whole(),
        out_shape=jax.ShapeDtypeStruct((count, tokens, width), BF16),
        scratch_shapes=[
            pltpu.SMEM((count,), jnp.int32),
            VMEM((count, tokens, width), BF16),
            VMEM((1, width), F32),
            VMEM((1, width), F32),
            pltpu.SemaphoreType.DMA((3 + count,)),
        ],
        compiler_params=params(60),
        cost_estimate=cost(10 * count * tokens * width, 4 * count * tokens * width),
        name="fetch",
    )(row_ids, pair_rep, ln_gain, ln_bias)


def bias_kernel(
    pair_rep, ln_gain, ln_bias, w_bias, pad_mask, out, rows, lifted, gain, shift, weights, live, sems
):
    heads, block, tokens = out.shape
    width = rows.shape[2]
    small = [(ln_gain, gain), (ln_bias, shift), (w_bias, weights), (pad_mask, live)]
    copies = [pltpu.make_async_copy(a, b, sems.at[i]) for i, (a, b) in enumerate(small)]
    for i in range(0, block, BIAS_ROWS):
        part = pl.ds(i, BIAS_ROWS)
        at = len(small) + i // BIAS_ROWS
        copies.append(pltpu.make_async_copy(pair_rep.at[part], rows.at[part], sems.at[at]))
    for copy in copies:
        copy.start()
    for copy in copies[: len(small)]:
        copy.wait()
    plain = weights[...].astype(F32)
    scaled = plain * gain[...]
    high = scaled.astype(BF16).astype(F32)
    at = lax.broadcasted_iota(jnp.int32, (heads * 8, width), 0) % 8
    offset = jnp.sum(plain * shift[...], axis=1, keepdims=True)
    offset = jnp.broadcast_to(offset[:, None], (heads, 8, tokens))
    for part, value in enumerate((high, scaled - high)):
        value = jnp.broadcast_to(value[:, None], (heads, 8, width)).reshape(heads * 8, width)
        for j in range(8):
            placed = jnp.where(at == j, value, 0.0).astype(BF16)
            at_j = slice(j * width, (j + 1) * width)
            lifted[part * heads * 8 : (part + 1) * heads * 8, at_j] = placed
    real = live[...] > 0
    sub = lax.broadcasted_iota(jnp.int32, (8, tokens), 0)

    def eight(group, carry):
        spread = jnp.zeros((8, tokens), F32)
        turned = []
        for j in range(8):
            values = rows[group * 8 + j].T.astype(F32)
            values = values - jnp.sum(values, axis=0, keepdims=True) * (1.0 / width)
            turned.append(values.astype(BF16))
            squares = jnp.sum(values * values, axis=0, keepdims=True)
            spread = jnp.where(sub == j, squares, spread)
        scale = lax.rsqrt(spread * (1.0 / width) + 1e-05)
        turned = jnp.concatenate(turned, axis=0)
        total = jnp.dot(lifted[...], turned, preferred_element_type=F32)
        total = total[: heads * 8] + total[heads * 8 :]
        total = total.reshape(heads, 8, tokens) * scale[None] + offset
        out[:, pl.ds(pl.multiple_of(group * 8, 8), 8), :] = jnp.where(real, total, MASKED)
        return carry

    for i in range(0, block, BIAS_ROWS):
        copies[len(small) + i // BIAS_ROWS].wait()
        lax.fori_loop(i // 8, (i + BIAS_ROWS) // 8, eight, 0)


def pair_bias(pair_rep, ln_gain, ln_bias, w_bias, pad_mask):
    block, tokens, width = pair_rep.shape
    heads = w_bias.shape[1]
    return pl.pallas_call(
        bias_kernel,
        in_specs=[pl.BlockSpec(memory_space=pltpu.HBM)] * 5,
        out_specs=whole(),
        out_shape=jax.ShapeDtypeStruct((heads, block, tokens), F32),
        scratch_shapes=[
            VMEM((block, tokens, width), BF16),
            VMEM((2 * heads * 8, 8 * width), BF16),
            VMEM((1, width), F32),
            VMEM((1, width), F32),
            VMEM((heads, width), BF16),
            VMEM((1, tokens), jnp.int32),
            pltpu.SemaphoreType.DMA((4 + block // BIAS_ROWS,)),
        ],
        compiler_params=params(60),
        cost_estimate=cost(4 * block * tokens * width, 2 * block * tokens * width),
        name="pair_bias",
    )(pair_rep, ln_gain, ln_bias, w_bias.T, pad_mask.reshape(1, tokens))


def project_kernel(*refs):
    blocks, (w_key, w_value, bias, keys, values, bias_near, sem) = refs[:4], refs[4:]
    copy = pltpu.make_async_copy(bias, bias_near, sem)
    copy.start()
    block, width = blocks[0].shape[-2:]
    row, col = lax.axis_index("row"), lax.axis_index("col")
    y, h, x, q = row // 4, row % 4, col // 4, col % 4
    places = [(x - y + s + 4) % 4 for s in range(4)]
    flips = [((h - i + 4) % 4) ^ q for i in range(4)]
    places += [(f // 2) + (f % 2) * 2 for f in flips]
    weights = jnp.concatenate([w_key[...], w_value[...]], axis=1)
    for s in range(4):
        for i in range(4):
            for t in range(2):
                both = jnp.dot(blocks[s][i, t], weights, preferred_element_type=F32)
                both = both.astype(BF16)
                at = pl.ds(pl.multiple_of(places[4 + i] * block, block), block)
                keys[places[s], t, :, at] = both[:, :width].T
                values[places[s], t, at, :] = both[:, width:]
    copy.wait()


def project(blocks, w_key, w_value, bias):
    block, width = blocks[0].shape[-2:]
    return pl.pallas_call(
        project_kernel,
        in_specs=[whole()] * 6 + [pl.BlockSpec(memory_space=pltpu.HBM)],
        out_specs=[whole()] * 3,
        out_shape=[
            jax.ShapeDtypeStruct((4, 2, width, 4 * block), BF16),
            jax.ShapeDtypeStruct((4, 2, 4 * block, width), BF16),
            jax.ShapeDtypeStruct(bias.shape, F32),
        ],
        scratch_shapes=[pltpu.SemaphoreType.DMA],
        compiler_params=params(),
        cost_estimate=cost(2 * 4096 * 128 * 256, 3 << 20),
        name="project",
    )(*blocks, w_key, w_value, bias)


def attend_kernel(v, rows, keys, values, bias_a, bias_b, bias_c, bias_d, w_query, *rest):
    block, width = rows.shape[1:]
    heads = bias_a.shape[0]
    head_dim = width // heads
    lane = lax.broadcasted_iota(jnp.int32, (block, width), 1)
    out = rest[-1]
    if len(rest) > 1:
        w_gate, gate_bias, gates, out = rest
        for t in range(2):
            gate = jnp.dot(rows[t], w_gate[...], preferred_element_type=F32) + gate_bias[...]
            gates[t] = jax.nn.sigmoid(gate).astype(BF16)
    for t in range(2):
        query = jnp.dot(rows[t], w_query[...], preferred_element_type=F32)
        query = (query * (head_dim**-0.5)).astype(BF16)
        key = keys[v, t]
        value = jnp.concatenate([values[v, t], jnp.ones((4 * block, width), BF16)], axis=1)
        summed = jnp.zeros((block, width), F32)
        stats = jnp.zeros((block, width), F32)
        for h in range(heads):
            mine = lane // head_dim == h
            part = jnp.where(mine, query, jnp.zeros_like(query))
            scores = jnp.dot(part, key, preferred_element_type=F32)
            bias = [bias_a[h], bias_b[h], bias_c[h], bias_d[h]]
            scores = scores + jnp.concatenate(bias, axis=1)
            peak = jnp.max(scores, axis=1, keepdims=True)
            expo = jnp.exp(scores - peak).astype(BF16)
            result = jnp.dot(expo, value, preferred_element_type=F32)
            summed = jnp.where(mine, result[:, :width], summed)
            total = result[:, width:]
            high = peak.astype(BF16).astype(F32)
            middle = (peak - high).astype(BF16).astype(F32)
            for i, column in enumerate((high, middle, peak - high - middle, total)):
                stats = jnp.where(lane == i * heads + h, column, stats)
        out[t, :block] = summed.astype(BF16)
        out[t, block:] = stats.T[:STATS].astype(BF16)


def attend(v, rows, keys, values, biases, w_query, gating=()):
    _, block, width = rows.shape
    shapes = [jax.ShapeDtypeStruct((2, block + STATS, width), BF16)]
    if gating:
        shapes.insert(0, jax.ShapeDtypeStruct(rows.shape, BF16))
    return pl.pallas_call(
        functools.partial(attend_kernel, v),
        in_specs=[whole()] * (8 + len(gating)),
        out_specs=[whole()] * len(shapes),
        out_shape=shapes,
        compiler_params=params(),
        cost_estimate=cost(8 * 2 * 128 * 512 * 128 * 2, 2 << 20, 2 * 4 * 128 * 512),
    )(rows, keys, values, *biases, w_query, *gating)


def finish_kernel(first, second, third, fourth, gates, w_out, out):
    block, width = gates.shape[1:]
    heads = STATS // 4
    head_dim = width // heads
    parts = (first, second, third, fourth)
    source = lax.broadcasted_iota(jnp.int32, (width, 4 * width), 0)
    target = lax.broadcasted_iota(jnp.int32, (width, 4 * width), 1) // head_dim
    meets = (source % STATS == target) & (source < 2 * STATS)
    spreading = jnp.where(meets, 1.0, 0.0).astype(BF16)
    for t in range(2):
        peaks, totals = [], []
        for part in parts:
            stats = part[t, block:].astype(F32)
            peaks.append(stats[:heads] + stats[heads : 2 * heads] + stats[2 * heads : 3 * heads])
            totals.append(stats[3 * heads :])
        overall = jnp.maximum(jnp.maximum(peaks[0], peaks[1]), jnp.maximum(peaks[2], peaks[3]))
        factors = [jnp.exp(peak - overall) for peak in peaks]
        whole_total = sum(f * total for f, total in zip(factors, totals))
        factors = jnp.concatenate([f / whole_total for f in factors], axis=0)
        high = factors.astype(BF16)
        low = (factors - high.astype(F32)).astype(BF16)
        padding = jnp.zeros((width - 2 * STATS, block), BF16)
        factors = jnp.concatenate([high, low, padding], axis=0).T
        wide = jnp.dot(factors, spreading, preferred_element_type=F32)
        attended = jnp.zeros((block, width), F32)
        for p, part in enumerate(parts):
            attended += wide[:, p * width : (p + 1) * width] * part[t, :block].astype(F32)
        gated = (gates[t].astype(F32) * attended).astype(BF16)
        out[t] = jnp.dot(gated, w_out[...], preferred_element_type=F32).astype(BF16)


def finish(parts, gates, w_out):
    return pl.pallas_call(
        finish_kernel,
        in_specs=[whole()] * 6,
        out_specs=whole(),
        out_shape=jax.ShapeDtypeStruct(gates.shape, BF16),
        compiler_params=params(),
        cost_estimate=cost(4 * 256 * 128 * 128, 1 << 19),
        name="finish",
    )(*parts, gates, w_out)


def moves(target):
    pairs = []
    for i in range(256):
        y, h, x, q = i // 64, i // 16 % 4, i // 4 % 4, i % 4
        a, b, c, d = target(y, h, x, q)
        pairs.append((i, ((a % 4 * 4 + b % 4) * 4 + c % 4) * 4 + d % 4))
    return pairs


def send(value, target):
    return lax.ppermute(value, AXES, moves(target))


def body(
    pair_rep,
    row_ids,
    pad_mask,
    ln_gain,
    ln_bias,
    w_query,
    w_key,
    w_value,
    w_gate,
    gate_bias,
    w_bias,
    w_out,
):
    _, _, width = pair_rep.shape
    ln_gain, ln_bias = ln_gain.reshape(1, width), ln_bias.reshape(1, width)
    piece = fetch(row_ids, pair_rep, ln_gain, ln_bias)
    low = []
    for i in range(4):
        low.append(send(piece, lambda y, h, x, q, i=i: (y, q + i, x, h)))

    bias = pair_bias(pair_rep, ln_gain, ln_bias, w_bias, pad_mask)
    bias_z = send(bias, lambda y, h, x, q: (y, h, x, q ^ 2))
    bias_c = send(bias, lambda y, h, x, q: (y, h, x, q ^ 1))
    bias_zc = send(bias_z, lambda y, h, x, q: (y, h, x, q ^ 1))

    own = jnp.stack(low)
    rows_kv = [own]
    for s in (1, 2, 3):
        rows_kv.append(send(own, lambda y, h, x, q, s=s: (y + s, h, x, q)))
    rows_q = []
    for s in range(4):
        rows_q.append(send(low[0], lambda y, h, x, q, s=s: (x, h, y + s, q)))

    keys, values, bias = project(rows_kv, w_key, w_value, bias)
    biases = (bias, bias_z, bias_c, bias_zc)
    parts = []
    for s in (2, 1, 3):
        (part,) = attend(s, rows_q[s], keys, values, biases, w_query)
        parts.append(send(part, lambda y, h, x, q, s=s: (y, h, x - s, q)))
    gating = (w_gate, gate_bias.reshape(1, width))
    gates, part = attend(0, rows_q[0], keys, values, biases, w_query, gating)
    return finish(parts + [part], gates, w_out)


def solution(mesh):
    return jax.shard_map(
        body,
        mesh=mesh,
        in_specs=(P("row", "col", None), P("row"), P("col")) + (P(),) * 9,
        out_specs=P("col", "row", None),
        check_vma=False,
    )
```

```python
import functools

import jax
import jax.numpy as jnp
from jax import lax
from jax.experimental import pallas as pl
from jax.experimental.pallas import tpu as pltpu
from jax.sharding import PartitionSpec as P


MASKED = -1e30
STATS = 16
BIAS_ROWS = 16
AXES = ("row", "col")
F32 = jnp.float32
BF16 = jnp.bfloat16
VMEM = pltpu.VMEM


def params(mib=16):
    return pltpu.CompilerParams(vmem_limit_bytes=mib << 20)


def cost(flops, moved, exps=0):
    return pl.CostEstimate(flops=flops, bytes_accessed=moved, transcendentals=exps)


def whole():
    return pl.BlockSpec(memory_space=VMEM)


def layer_norm(values, ln_gain, ln_bias):
    values = values.astype(F32)
    values = values - jnp.mean(values, axis=-1, keepdims=True)
    spread = jnp.mean(values * values, axis=-1, keepdims=True)
    return (values * lax.rsqrt(spread + 1e-05) * ln_gain + ln_bias).astype(BF16)


def fetch_kernel(row_ids, pair_rep, ln_gain, ln_bias, out, ids, rows, gain, shift, sems):
    copies = [
        pltpu.make_async_copy(row_ids, ids, sems.at[0]),
        pltpu.make_async_copy(ln_gain, gain, sems.at[1]),
        pltpu.make_async_copy(ln_bias, shift, sems.at[2]),
    ]
    for copy in copies:
        copy.start()
    copies[0].wait()
    for t in range(rows.shape[0]):
        at = lax.rem(ids[t], pair_rep.shape[0])
        copies.append(pltpu.make_async_copy(pair_rep.at[at], rows.at[t], sems.at[3 + t]))
        copies[-1].start()
    copies[1].wait()
    copies[2].wait()
    for t in range(rows.shape[0]):
        copies[3 + t].wait()
        out[t] = layer_norm(rows[t], gain[...], shift[...])


def fetch(row_ids, pair_rep, ln_gain, ln_bias):
    _, tokens, width = pair_rep.shape
    count = row_ids.shape[0]
    return pl.pallas_call(
        fetch_kernel,
        in_specs=[pl.BlockSpec(memory_space=pltpu.HBM)] * 4,
        out_specs=whole(),
        out_shape=jax.ShapeDtypeStruct((count, tokens, width), BF16),
        scratch_shapes=[
            pltpu.SMEM((count,), jnp.int32),
            VMEM((count, tokens, width), BF16),
            VMEM((1, width), F32),
            VMEM((1, width), F32),
            pltpu.SemaphoreType.DMA((3 + count,)),
        ],
        compiler_params=params(60),
        cost_estimate=cost(10 * count * tokens * width, 4 * count * tokens * width),
        name="fetch",
    )(row_ids, pair_rep, ln_gain, ln_bias)


def bias_kernel(
    pair_rep, ln_gain, ln_bias, w_bias, pad_mask, out, rows, lifted, gain, shift, weights, live, sems
):
    heads, block, tokens = out.shape
    width = rows.shape[2]
    small = [(ln_gain, gain), (ln_bias, shift), (w_bias, weights), (pad_mask, live)]
    copies = [pltpu.make_async_copy(a, b, sems.at[i]) for i, (a, b) in enumerate(small)]
    for i in range(0, block, BIAS_ROWS):
        part = pl.ds(i, BIAS_ROWS)
        at = len(small) + i // BIAS_ROWS
        copies.append(pltpu.make_async_copy(pair_rep.at[part], rows.at[part], sems.at[at]))
    for copy in copies:
        copy.start()
    for copy in copies[: len(small)]:
        copy.wait()
    plain = weights[...].astype(F32)
    scaled = plain * gain[...]
    high = scaled.astype(BF16).astype(F32)
    at = lax.broadcasted_iota(jnp.int32, (heads * 8, width), 0) % 8
    offset = jnp.sum(plain * shift[...], axis=1, keepdims=True)
    offset = jnp.broadcast_to(offset[:, None], (heads, 8, tokens))
    for part, value in enumerate((high, scaled - high)):
        value = jnp.broadcast_to(value[:, None], (heads, 8, width)).reshape(heads * 8, width)
        for j in range(8):
            placed = jnp.where(at == j, value, 0.0).astype(BF16)
            at_j = slice(j * width, (j + 1) * width)
            lifted[part * heads * 8 : (part + 1) * heads * 8, at_j] = placed
    real = live[...] > 0
    sub = lax.broadcasted_iota(jnp.int32, (8, tokens), 0)

    def eight(group, carry):
        spread = jnp.zeros((8, tokens), F32)
        turned = []
        for j in range(8):
            values = rows[group * 8 + j].T.astype(F32)
            values = values - jnp.sum(values, axis=0, keepdims=True) * (1.0 / width)
            turned.append(values.astype(BF16))
            squares = jnp.sum(values * values, axis=0, keepdims=True)
            spread = jnp.where(sub == j, squares, spread)
        scale = lax.rsqrt(spread * (1.0 / width) + 1e-05)
        turned = jnp.concatenate(turned, axis=0)
        total = jnp.dot(lifted[...], turned, preferred_element_type=F32)
        total = total[: heads * 8] + total[heads * 8 :]
        total = total.reshape(heads, 8, tokens) * scale[None] + offset
        out[:, pl.ds(pl.multiple_of(group * 8, 8), 8), :] = jnp.where(real, total, MASKED)
        return carry

    for i in range(0, block, BIAS_ROWS):
        copies[len(small) + i // BIAS_ROWS].wait()
        lax.fori_loop(i // 8, (i + BIAS_ROWS) // 8, eight, 0)


def pair_bias(pair_rep, ln_gain, ln_bias, w_bias, pad_mask):
    block, tokens, width = pair_rep.shape
    heads = w_bias.shape[1]
    return pl.pallas_call(
        bias_kernel,
        in_specs=[pl.BlockSpec(memory_space=pltpu.HBM)] * 5,
        out_specs=whole(),
        out_shape=jax.ShapeDtypeStruct((heads, block, tokens), F32),
        scratch_shapes=[
            VMEM((block, tokens, width), BF16),
            VMEM((2 * heads * 8, 8 * width), BF16),
            VMEM((1, width), F32),
            VMEM((1, width), F32),
            VMEM((heads, width), BF16),
            VMEM((1, tokens), jnp.int32),
            pltpu.SemaphoreType.DMA((4 + block // BIAS_ROWS,)),
        ],
        compiler_params=params(52),
        cost_estimate=cost(4 * block * tokens * width, 2 * block * tokens * width),
        name="pair_bias",
    )(pair_rep, ln_gain, ln_bias, w_bias.T, pad_mask.reshape(1, tokens))


def project_kernel(*refs):
    blocks, (w_key, w_value, keys, values) = refs[:4], refs[4:]
    block, width = blocks[0].shape[-2:]
    row, col = lax.axis_index("row"), lax.axis_index("col")
    y, h, x, q = row // 4, row % 4, col // 4, col % 4
    places = [(x - y + s + 4) % 4 for s in range(4)]
    flips = [((h - i + 4) % 4) ^ q for i in range(4)]
    places += [(f // 2) + (f % 2) * 2 for f in flips]
    weights = jnp.concatenate([w_key[...], w_value[...]], axis=1)
    for s in range(4):
        for i in range(4):
            for t in range(2):
                both = jnp.dot(blocks[s][i, t], weights, preferred_element_type=F32)
                both = both.astype(BF16)
                at = pl.ds(pl.multiple_of(places[4 + i] * block, block), block)
                keys[places[s], t, :, at] = both[:, :width].T
                values[places[s], t, at, :] = both[:, width:]


def project(blocks, w_key, w_value):
    block, width = blocks[0].shape[-2:]
    return pl.pallas_call(
        project_kernel,
        in_specs=[whole()] * 6,
        out_specs=[whole()] * 2,
        out_shape=[
            jax.ShapeDtypeStruct((4, 2, width, 4 * block), BF16),
            jax.ShapeDtypeStruct((4, 2, 4 * block, width), BF16),
        ],
        compiler_params=params(),
        cost_estimate=cost(2 * 4096 * 128 * 256, 3 << 20),
        name="project",
    )(*blocks, w_key, w_value)


def attend_kernel(v, rows, keys, values, bias_a, bias_b, bias_c, bias_d, w_query, *rest):
    block, width = rows.shape[1:]
    heads = bias_a.shape[0]
    head_dim = width // heads
    lane = lax.broadcasted_iota(jnp.int32, (block, width), 1)
    out = rest[-1]
    if len(rest) > 1:
        w_gate, gate_bias, gates, out = rest
        for t in range(2):
            gate = jnp.dot(rows[t], w_gate[...], preferred_element_type=F32) + gate_bias[...]
            gates[t] = jax.nn.sigmoid(gate).astype(BF16)
    for t in range(2):
        query = jnp.dot(rows[t], w_query[...], preferred_element_type=F32)
        query = (query * (head_dim**-0.5)).astype(BF16)
        key = keys[v, t]
        value = jnp.concatenate([values[v, t], jnp.ones((4 * block, width), BF16)], axis=1)
        summed = jnp.zeros((block, width), F32)
        stats = jnp.zeros((block, width), F32)
        for h in range(heads):
            mine = lane // head_dim == h
            part = jnp.where(mine, query, jnp.zeros_like(query))
            scores = jnp.dot(part, key, preferred_element_type=F32)
            bias = [bias_a[h], bias_b[h], bias_c[h], bias_d[h]]
            scores = scores + jnp.concatenate(bias, axis=1)
            peak = jnp.max(scores, axis=1, keepdims=True)
            expo = jnp.exp(scores - peak).astype(BF16)
            result = jnp.dot(expo, value, preferred_element_type=F32)
            summed = jnp.where(mine, result[:, :width], summed)
            total = result[:, width:]
            high = peak.astype(BF16).astype(F32)
            middle = (peak - high).astype(BF16).astype(F32)
            for i, column in enumerate((high, middle, peak - high - middle, total)):
                stats = jnp.where(lane == i * heads + h, column, stats)
        out[t, :block] = summed.astype(BF16)
        out[t, block:] = stats.T[:STATS].astype(BF16)


def attend(v, rows, keys, values, biases, w_query, gating=()):
    _, block, width = rows.shape
    shapes = [jax.ShapeDtypeStruct((2, block + STATS, width), BF16)]
    if gating:
        shapes.insert(0, jax.ShapeDtypeStruct(rows.shape, BF16))
    return pl.pallas_call(
        functools.partial(attend_kernel, v),
        in_specs=[whole()] * (8 + len(gating)),
        out_specs=[whole()] * len(shapes),
        out_shape=shapes,
        compiler_params=params(),
        cost_estimate=cost(8 * 2 * 128 * 512 * 128 * 2, 2 << 20, 2 * 4 * 128 * 512),
    )(rows, keys, values, *biases, w_query, *gating)


def finish_kernel(first, second, third, fourth, gates, w_out, out):
    block, width = gates.shape[1:]
    heads = STATS // 4
    head_dim = width // heads
    parts = (first, second, third, fourth)
    source = lax.broadcasted_iota(jnp.int32, (width, 4 * width), 0)
    target = lax.broadcasted_iota(jnp.int32, (width, 4 * width), 1) // head_dim
    meets = (source % STATS == target) & (source < 2 * STATS)
    spreading = jnp.where(meets, 1.0, 0.0).astype(BF16)
    for t in range(2):
        peaks, totals = [], []
        for part in parts:
            stats = part[t, block:].astype(F32)
            peaks.append(stats[:heads] + stats[heads : 2 * heads] + stats[2 * heads : 3 * heads])
            totals.append(stats[3 * heads :])
        overall = jnp.maximum(jnp.maximum(peaks[0], peaks[1]), jnp.maximum(peaks[2], peaks[3]))
        factors = [jnp.exp(peak - overall) for peak in peaks]
        whole_total = sum(f * total for f, total in zip(factors, totals))
        factors = jnp.concatenate([f / whole_total for f in factors], axis=0)
        high = factors.astype(BF16)
        low = (factors - high.astype(F32)).astype(BF16)
        padding = jnp.zeros((width - 2 * STATS, block), BF16)
        factors = jnp.concatenate([high, low, padding], axis=0).T
        wide = jnp.dot(factors, spreading, preferred_element_type=F32)
        attended = jnp.zeros((block, width), F32)
        for p, part in enumerate(parts):
            attended += wide[:, p * width : (p + 1) * width] * part[t, :block].astype(F32)
        gated = (gates[t].astype(F32) * attended).astype(BF16)
        out[t] = jnp.dot(gated, w_out[...], preferred_element_type=F32).astype(BF16)


def finish(parts, gates, w_out):
    return pl.pallas_call(
        finish_kernel,
        in_specs=[whole()] * 6,
        out_specs=whole(),
        out_shape=jax.ShapeDtypeStruct(gates.shape, BF16),
        compiler_params=params(),
        cost_estimate=cost(4 * 256 * 128 * 128, 1 << 19),
        name="finish",
    )(*parts, gates, w_out)


def moves(target):
    pairs = []
    for i in range(256):
        y, h, x, q = i // 64, i // 16 % 4, i // 4 % 4, i % 4
        a, b, c, d = target(y, h, x, q)
        pairs.append((i, ((a % 4 * 4 + b % 4) * 4 + c % 4) * 4 + d % 4))
    return pairs


def send(value, target):
    return lax.ppermute(value, AXES, moves(target))


def body(
    pair_rep,
    row_ids,
    pad_mask,
    ln_gain,
    ln_bias,
    w_query,
    w_key,
    w_value,
    w_gate,
    gate_bias,
    w_bias,
    w_out,
):
    _, _, width = pair_rep.shape
    ln_gain, ln_bias = ln_gain.reshape(1, width), ln_bias.reshape(1, width)
    piece = fetch(row_ids, pair_rep, ln_gain, ln_bias)
    low = []
    for i in range(4):
        low.append(send(piece, lambda y, h, x, q, i=i: (y, q + i, x, h)))

    bias = pair_bias(pair_rep, ln_gain, ln_bias, w_bias, pad_mask)
    bias_z = send(bias, lambda y, h, x, q: (y, h, x, q ^ 2))
    bias_c = send(bias, lambda y, h, x, q: (y, h, x, q ^ 1))
    bias_zc = send(bias_z, lambda y, h, x, q: (y, h, x, q ^ 1))

    own = jnp.stack(low)
    rows_kv = [own]
    for s in (1, 2, 3):
        rows_kv.append(send(own, lambda y, h, x, q, s=s: (y + s, h, x, q)))
    rows_q = []
    for s in range(4):
        rows_q.append(send(low[0], lambda y, h, x, q, s=s: (x, h, y + s, q)))

    keys, values = project(rows_kv, w_key, w_value)
    biases = (bias, bias_z, bias_c, bias_zc)
    parts = []
    for s in (3, 1, 2):
        (part,) = attend(s, rows_q[s], keys, values, biases, w_query)
        parts.append(send(part, lambda y, h, x, q, s=s: (y, h, x - s, q)))
    gating = (w_gate, gate_bias.reshape(1, width))
    gates, part = attend(0, rows_q[0], keys, values, biases, w_query, gating)
    return finish(parts + [part], gates, w_out)


def solution(mesh):
    return jax.shard_map(
        body,
        mesh=mesh,
        in_specs=(P("row", "col", None), P("row"), P("col")) + (P(),) * 9,
        out_specs=P("col", "row", None),
        check_vma=False,
    )
```
